32 devices in a mesh: seq: 8 (over z, x), hid: 4 (over y, core).
Axes of the slice: x: 2, y: 2, z: 4, core: 2. Of those that a mesh axis runs over, the one named last changes fastest.
Arguments:
- hidden: bfloat16 [8192, 4096], P('seq', 'hid'), may hold values from -40 to 40, as said below
- seg_ids: int32 [8192], P('seq'), may hold values from 0 to 31, as said below
- lengths: int32 [32], replicated, may hold values from 64 to 4096, as said below
- owner_slot: int32 [32], replicated, may hold values from 0 to 31, each once
- pool_bias: float32 [4096], P('hid'), may hold values from -3 to 3
Outputs:
- pooled: bfloat16 [32, 4096], P('seq', 'hid')
The draws below stay inside these ranges and needn't reach their ends.
Inputs may be any that keep to these rules, and one draw needn't show every extreme that they name: `hidden`: float values; each feature's scale differs. `seg_ids`: never falls along the stream; document d occupies exactly lengths[d] consecutive tokens, documents in order. `lengths`: they sum to 8192; one of them is exactly 4096; the first 16 documents each have 1024 // 16 tokens and so fill the first index's tokens; hence at most 16 documents end within one index's tokens, and the first index has exactly 16. `owner_slot`: each row number once.
All inputs are finite; a program needn't handle non-finite values.
Results may differ from the reference program's by a relative error of at most 0.001.
Values may be sent and summed in bfloat16 or wider, within the bound.
A program may use at most 64 MiB of HBM per device.

```python
import math
import jax
import jax.numpy as jnp
from jax import lax

D = 4096
TOK_DEV = 1024
FIN = 16
TOKENS = 8192
DOCS = 32
MOST = 4096
N_SEQ = 8


def doc_lengths(key):
    floor_size = TOK_DEV // FIN
    remaining = TOKENS - MOST - TOK_DEV
    others = DOCS - 1 - FIN
    even_share = remaining // others
    leftover = remaining % others
    positions = jnp.arange(others, dtype=jnp.int32)
    doc_sizes = even_share + (positions < leftover).astype(jnp.int32)
    pair_count = others // 2
    for sweep_index in range(6):
        key, pair_key, move_key = jax.random.split(key, 3)
        shuffled = jax.random.permutation(pair_key, others).astype(jnp.int32)
        giver = shuffled[0:2 * pair_count:2]
        taker = shuffled[1:2 * pair_count:2]
        headroom = jnp.minimum(doc_sizes[giver] - floor_size, MOST - doc_sizes[taker])
        transfer = jax.random.randint(move_key, (pair_count,), 0, headroom + 1).astype(jnp.int32)
        doc_sizes = doc_sizes.at[giver].add(-transfer).at[taker].add(transfer)
    tail_count = others + 1
    long_index = jax.random.randint(key, (), 0, tail_count).astype(jnp.int32)
    tail_iota = jnp.arange(tail_count, dtype=jnp.int32)
    shifted = jnp.clip(jnp.where(tail_iota < long_index, tail_iota, tail_iota - 1), 0, others - 1)
    tail = jnp.where(tail_iota == long_index, MOST, doc_sizes[shifted])
    head = jnp.full((FIN,), floor_size, jnp.int32)
    return jnp.concatenate([head, tail.astype(jnp.int32)]).astype(jnp.int32)


def draw_lengths(key, part):
    return doc_lengths(jax.random.fold_in(key, 11))


def draw_seg_ids(key, part):
    sizes_drawn = doc_lengths(jax.random.fold_in(key, 11))
    starts = jnp.cumsum(sizes_drawn) - sizes_drawn
    marks = jnp.zeros((TOKENS,), jnp.int32).at[starts[1:]].add(1)
    return jnp.cumsum(marks).astype(jnp.int32)


def draw_hidden(key, part):
    col_key = jax.random.fold_in(key, 0)
    value_key = jax.random.fold_in(key, 2)
    rising = jnp.exp2(jnp.arange(D, dtype=jnp.float32) / D)
    columns = jnp.exp(jax.random.uniform(col_key, (D,), jnp.float32, math.log(0.7), math.log(1.4)))
    values = jnp.clip(jax.random.normal(value_key, (TOKENS, D), jnp.float32), -4.0, 4.0)
    result = values * (columns * rising)[None, :]
    return result.astype(jnp.bfloat16)


def shard_levels(own_key, shape, cuts, least, high):
    def one(axis_at, shards_of):
        steps = jax.random.uniform(jax.random.fold_in(jax.random.fold_in(own_key, 6), axis_at), (shards_of,), jnp.float32, least / len(cuts), high / len(cuts))
        return jnp.repeat(jnp.exp(steps), shape[axis_at] // shards_of).reshape((-1,) + (1,) * (len(shape) - axis_at - 1))

    loudness = one(*cuts[0])
    for cut in cuts[1:]:
        loudness = loudness * one(*cut)
    return loudness


def centred(own_key, dims, scale, limit, pieces=(), kind=jnp.bfloat16):
    values = jax.random.normal(own_key, dims, jnp.float32) * scale
    if len(pieces) > 0:
        values = shard_levels(own_key, dims, pieces, -0.22, 0.18) * values
    return jnp.clip(values, min=-limit, max=limit).astype(kind)


def setup_inputs(seed: int = 0) -> dict:
    key_list = jax.random.split(jax.random.key(seed), 6)
    hidden = draw_hidden(jax.random.fold_in(key_list[5], 71), 0)
    seg_ids = draw_seg_ids(jax.random.fold_in(key_list[5], 71), 0)
    lengths = draw_lengths(jax.random.fold_in(key_list[5], 71), 0)
    owner_slot = jax.random.permutation(key_list[3], DOCS).astype(jnp.int32)
    pool_bias = centred(key_list[4], (D,), 0.5, 3.0, ((0, 4),), jnp.float32)
    return {"hidden": hidden, "seg_ids": seg_ids, "lengths": lengths, "owner_slot": owner_slot, "pool_bias": pool_bias}


def reference(hidden, seg_ids, lengths, owner_slot, pool_bias):
    token_blocks = hidden.reshape(N_SEQ, TOK_DEV, D)
    block_ids = seg_ids.reshape(N_SEQ, TOK_DEV)

    def accumulate(running, operands):
        token_block, block_docs = operands
        added = jax.ops.segment_sum(token_block.astype(jnp.float32), block_docs, num_segments=DOCS)
        return (running + added, None)
    totals, _ = lax.scan(accumulate, jnp.zeros((DOCS, D), jnp.float32), (token_blocks, block_ids))
    averages = totals / lengths.astype(jnp.float32)[:, None] + pool_bias[None, :]
    energy = lax.optimization_barrier(jnp.mean(averages * averages, axis=1, keepdims=True))
    normed = averages * lax.rsqrt(energy + 1e-06)
    placed = jnp.zeros((DOCS, D), jnp.float32).at[owner_slot].set(normed)
    return placed.astype(jnp.bfloat16)
```

```python
import functools

import jax
import jax.numpy as jnp
from jax import lax
from jax.experimental import pallas as pl
from jax.experimental.pallas import tpu as pltpu
from jax.sharding import PartitionSpec as P

MESH = pl.DeviceIdType.MESH
LANES = 128
STEPS = 32.0
TOP = 32700.0


def widened(code):
    tiles = code.shape[1] // LANES - 1
    value = code.astype(jnp.int32).astype(jnp.float32)
    unit = jnp.exp2(value[:, tiles * LANES :] * (1.0 / STEPS)) * (1.0 / TOP)
    return [value[:, j * LANES : (j + 1) * LANES] * unit for j in range(tiles)]


def summed(land, group):
    total = widened(land[group, 0])
    for k in range(1, land.shape[1]):
        total = [a + b for a, b in zip(total, widened(land[group, k]))]
    return total


def squared(tiles):
    out = tiles[0] * tiles[0]
    for t in tiles[1:]:
        out = out + t * t
    return out


def kernel(
    n_seq, n_hid, pair, fold, chunks,
    hidden_hbm, seg_hbm, len_hbm, slot_hbm, bias_hbm,
    out_ref,
    hidden, seg, lens, slots, bias, code, land, extra, mine, theirs,
    load_sems, small_sems, send_sems, recv_sems, extra_send, extra_recv, sq_send, sq_recv,
):
    me = lax.axis_index("seq")
    my_hid = lax.axis_index("hid")
    tokens, width = hidden.shape
    docs = lens.shape[1]
    per_owner = docs // n_seq
    block = per_owner * fold
    part = width // fold
    groups = n_hid // pair
    low = lax.rem(my_hid, pair)
    high = my_hid // pair
    features = width * n_hid
    peers = [jnp.where(j < me, j, j + 1) for j in range(n_seq - 1)]

    rows = tokens // chunks
    smalls = [
        pltpu.make_async_copy(src, dst, small_sems.at[i])
        for i, (src, dst) in enumerate(
            ((slot_hbm, slots), (seg_hbm, seg), (len_hbm, lens), (bias_hbm, bias))
        )
    ]
    loads = [
        pltpu.make_async_copy(
            hidden_hbm.at[pl.ds(t * rows, rows), :], hidden.at[pl.ds(t * rows, rows), :], load_sems.at[t]
        )
        for t in range(chunks)
    ]
    for c in smalls:
        c.start()
    for c in loads:
        c.start()

    barrier = pltpu.get_barrier_semaphore()

    def greet(seq, hid):
        pl.semaphore_signal(barrier, inc=1, device_id=(seq, hid), device_id_type=MESH)

    greeted = 0
    for g in range(groups):
        hid = low + pair * lax.rem(high + g, groups)
        for p in peers:
            greet(p, hid)
            greeted += 1
        if g > 0:
            greet(me, hid)
            greeted += 1
    if pair == 2:
        greet(me, my_hid + 1 - 2 * low)
        greeted += 1

        @pl.when((me == 0) & (my_hid == 1))
        def _():
            for p in range(n_seq):
                for g in range(groups):
                    greet(p, pair * g)

    smalls[0].wait()
    row = lax.broadcasted_iota(jnp.int32, (n_seq * block, 1), 0)
    inner = lax.rem(row, block)
    row_slot = (row // block) * per_owner + lax.rem(inner, per_owner)
    row_part = inner // per_owner
    doc = lax.broadcasted_iota(jnp.int32, (1, docs), 1)
    here = row_slot == slots[...]
    row_doc = jnp.sum(jnp.where(here, doc.astype(jnp.float32), 0.0), axis=1, keepdims=True).astype(jnp.int32)
    smalls[1].wait()
    pickers = [
        jnp.concatenate(
            [
                jnp.where(
                    jnp.where(row_part == f, row_doc, -1) == seg[k : k + 1, :], 1.0, 0.0
                ).astype(jnp.bfloat16)
                for k in range(tokens // LANES)
            ],
            axis=1,
        )
        for f in range(fold)
    ]
    smalls[2].wait()
    smalls[3].wait()
    length = lens[...].astype(jnp.float32)
    row_len = jnp.sum(jnp.where(here, length, 0.0), axis=1, keepdims=True)
    row_first = jnp.sum(jnp.where(doc < row_doc, length, 0.0), axis=1, keepdims=True)
    first = (me * tokens).astype(jnp.float32)
    starts = jnp.where((row_first >= first) & (row_first < first + tokens), 1.0, 0.0)
    inverse = 1.0 / row_len
    block_part = lax.broadcasted_iota(jnp.int32, (block, 1), 0) // per_owner
    offset = bias[:, :part]
    for f in range(1, fold):
        offset = jnp.where(block_part == f, bias[:, f * part : (f + 1) * part], offset)

    sums = None
    for t in range(chunks):
        loads[t].wait()
        for f in range(fold):
            term = jnp.dot(
                pickers[f][:, t * rows : (t + 1) * rows],
                hidden[t * rows : (t + 1) * rows, f * part : (f + 1) * part],
                preferred_element_type=jnp.float32,
            )
            sums = term if sums is None else sums + term

    for p in range(n_seq):
        at = slice(p * block, (p + 1) * block)
        share = sums[at] * inverse[at] + starts[at] * offset
        largest = jnp.abs(share[:, :LANES])
        for j in range(1, part // LANES):
            largest = jnp.maximum(largest, jnp.abs(share[:, j * LANES : (j + 1) * LANES]))
        step = jnp.ceil(jnp.log2(jnp.maximum(largest, 1e-30)) * STEPS)
        gain = jnp.exp2(step * (-1.0 / STEPS)) * TOP
        for j in range(part // LANES):
            lanes = slice(j * LANES, (j + 1) * LANES)
            code[p, :, lanes] = jnp.round(share[:, lanes] * gain).astype(jnp.int32).astype(jnp.int16)
        code[p, :, part:] = step.astype(jnp.int32).astype(jnp.int16)

    pl.semaphore_wait(barrier, greeted + jnp.where(low == 0, pair - 1, 0))

    def send(p, hid, g):
        pltpu.make_async_remote_copy(
            src_ref=code.at[p],
            dst_ref=land.at[g, me],
            send_sem=send_sems.at[g],
            recv_sem=recv_sems.at[g],
            device_id=(p, hid),
            device_id_type=MESH,
        ).start()

    for j, p in enumerate(peers):
        for i in range(groups):
            send(p, low + pair * i, lax.rem(high - i + groups, groups))
            if j == 0 and i == 0 and pair == 2:

                @pl.when(low == 0)
                def _():
                    pltpu.make_async_remote_copy(
                        src_ref=code.at[0],
                        dst_ref=extra.at[high, me],
                        send_sem=extra_send,
                        recv_sem=extra_recv,
                        device_id=(0, 1),
                        device_id_type=MESH,
                    ).start()
    for g in range(1, groups):
        send(me, low + pair * lax.rem(high + g, groups), groups - g)
    land[0, me] = code[me]

    most = land.at[0, pl.ds(0, n_seq - 1)]
    pltpu.make_async_copy(most, most, recv_sems.at[0]).wait()
    averages = summed(land, 0)
    lane_sq = squared(averages)
    for g in range(1, groups):
        pltpu.make_async_copy(land.at[g], land.at[g], recv_sems.at[g]).wait()
        lane_sq = lane_sq + squared(summed(land, g))

    if pair == 2:
        ahead = (me == 0) & (my_hid == 0)
        alone = (me == 0) & (my_hid == 1)
        mine[...] = lane_sq

        @pl.when(jnp.logical_not(ahead))
        def _():
            pltpu.make_async_remote_copy(
                src_ref=mine,
                dst_ref=theirs,
                send_sem=sq_send,
                recv_sem=sq_recv,
                device_id=(me, my_hid + 1 - 2 * low),
                device_id_type=MESH,
            ).start()

        @pl.when(alone)
        def _():
            pltpu.make_async_copy(extra, extra, extra_recv).wait()
            rest = squared(summed(extra, 0))
            for g in range(1, groups):
                rest = rest + squared(summed(extra, g))
            theirs[...] = rest

        @pl.when(jnp.logical_not(alone))
        def _():
            pltpu.make_async_copy(theirs, theirs, sq_recv).wait()

        lane_sq = lane_sq + theirs[...]

    energy = jnp.sum(lane_sq, axis=1, keepdims=True)
    total = energy[:per_owner]
    for f in range(1, fold):
        total = total + energy[f * per_owner : (f + 1) * per_owner]
    scale = lax.rsqrt(total / features + 1e-06)
    for f in range(fold):
        for j, tile in enumerate(averages):
            at = f * part + j * LANES
            out_ref[:, at : at + LANES] = (tile[f * per_owner : (f + 1) * per_owner] * scale).astype(jnp.bfloat16)

    pltpu.make_async_copy(most, most, send_sems.at[0]).wait()
    for g in range(1, groups):
        pltpu.make_async_copy(land.at[g], land.at[g], send_sems.at[g]).wait()
    if pair == 2:

        @pl.when(low == 0)
        def _():
            pltpu.make_async_copy(code.at[0], code.at[0], extra_send).wait()

        @pl.when(jnp.logical_not(ahead))
        def _():
            pltpu.make_async_copy(mine, mine, sq_send).wait()


def local(n_seq, n_hid, hidden, seg_ids, lengths, owner_slot, pool_bias):
    tokens, width = hidden.shape
    docs = lengths.shape[0]
    per_owner = docs // n_seq
    fold = max(1, 8 // per_owner)
    pair = 2 if n_hid % 2 == 0 else 1
    groups = n_hid // pair
    block, part = per_owner * fold, width // fold
    chunks = 4
    f32, i32, i16 = jnp.float32, jnp.int32, jnp.int16
    dma = pltpu.SemaphoreType.DMA
    vmem = pltpu.VMEM
    return pl.pallas_call(
        functools.partial(kernel, n_seq, n_hid, pair, fold, chunks),
        out_shape=vmem((per_owner, width), jnp.bfloat16),
        in_specs=[pl.BlockSpec(memory_space=pl.ANY)] * 5,
        out_specs=pl.BlockSpec(memory_space=vmem),
        scratch_shapes=[
            vmem((tokens, width), jnp.bfloat16),
            vmem((tokens // LANES, LANES), i32),
            vmem((1, docs), i32),
            vmem((1, docs), i32),
            vmem((1, width), f32),
            vmem((n_seq, block, part + LANES), i16),
            vmem((groups, n_seq, block, part + LANES), i16),
            vmem((groups, n_seq, block, part + LANES), i16),
            vmem((block, LANES), f32),
            vmem((block, LANES), f32),
            dma((chunks,)),
            dma((4,)),
            dma((groups,)),
            dma((groups,)),
            dma(()),
            dma(()),
            dma(()),
            dma(()),
        ],
        compiler_params=pltpu.CompilerParams(collective_id=0, has_side_effects=True),
    )(
        hidden,
        seg_ids.reshape(tokens // LANES, LANES),
        lengths.reshape(1, docs),
        owner_slot.reshape(1, docs),
        pool_bias.reshape(1, width),
    )


def solution(mesh):
    placed = (P("seq", "hid"), P("seq"), P(), P(), P("hid"))
    return jax.shard_map(
        functools.partial(local, mesh.shape["seq"], mesh.shape["hid"]),
        mesh=mesh,
        in_specs=placed,
        out_specs=P("seq", "hid"),
        check_vma=False,
    )
```

```python
import functools

import jax
import jax.numpy as jnp
from jax import lax
from jax.experimental import pallas as pl
from jax.experimental.pallas import tpu as pltpu
from jax.sharding import PartitionSpec as P

MESH = pl.DeviceIdType.MESH
LANES = 128
STEPS = 8.0
LEAST = 20.0
STEP_BITS = 8


def widened(code):
    tiles = code.shape[1] // LANES
    low = -(-STEP_BITS // tiles)
    top = float((1 << (15 - low)) - 24)
    words = [code[:, j * LANES : (j + 1) * LANES].astype(jnp.int32) for j in range(tiles)]
    step = words[0] & ((1 << low) - 1)
    for j in range(1, tiles):
        step = step | ((words[j] & ((1 << low) - 1)) << (low * j))
    unit = jnp.exp2(step.astype(jnp.float32) * (1.0 / STEPS) - LEAST) * (1.0 / top)
    return [(w >> low).astype(jnp.float32) * unit for w in words]


def narrowed(share):
    tiles = share.shape[1] // LANES
    low = -(-STEP_BITS // tiles)
    top = float((1 << (15 - low)) - 24)
    parts = [share[:, j * LANES : (j + 1) * LANES] for j in range(tiles)]
    largest = jnp.abs(parts[0])
    for x in parts[1:]:
        largest = jnp.maximum(largest, jnp.abs(x))
    step = jnp.ceil((jnp.log2(jnp.maximum(largest, 2.0**-LEAST)) + LEAST) * STEPS)
    gain = jnp.exp2(LEAST - step * (1.0 / STEPS)) * top
    bits = step.astype(jnp.int32)
    return [
        (
            (jnp.round(x * gain).astype(jnp.int32) << low) | ((bits >> (low * j)) & ((1 << low) - 1))
        ).astype(jnp.int16)
        for j, x in enumerate(parts)
    ]


def summed(land, group):
    total = widened(land[group, 0])
    for k in range(1, land.shape[1]):
        total = [a + b for a, b in zip(total, widened(land[group, k]))]
    return total


def squared(tiles):
    out = tiles[0] * tiles[0]
    for t in tiles[1:]:
        out = out + t * t
    return out


def kernel(
    n_seq, n_hid, pair, fold, chunks, direct,
    hidden_hbm, seg_hbm, len_hbm, slot_hbm, bias_hbm,
    out_ref,
    hidden, seg, lens, slots, bias, code, land, extra, mine, theirs, whole,
    load_sems, small_sems, send_sems, recv_sems, extra_send, extra_recv, sq_send, sq_recv,
):
    me = lax.axis_index("seq")
    my_hid = lax.axis_index("hid")
    tokens, width = hidden.shape
    docs = lens.shape[1]
    per_owner = docs // n_seq
    block = per_owner * fold
    part = width // fold
    groups = n_hid // pair
    low = lax.rem(my_hid, pair)
    high = my_hid // pair
    features = width * n_hid

    rows = tokens // chunks
    smalls = [
        pltpu.make_async_copy(src, dst, small_sems.at[i])
        for i, (src, dst) in enumerate(
            ((slot_hbm, slots), (seg_hbm, seg), (len_hbm, lens), (bias_hbm, bias))
        )
    ]
    loads = [
        pltpu.make_async_copy(
            hidden_hbm.at[pl.ds(t * rows, rows), :], hidden.at[pl.ds(t * rows, rows), :], load_sems.at[t]
        )
        for t in range(chunks)
    ]
    for c in smalls:
        c.start()
    for c in loads:
        c.start()

    barrier = pltpu.get_barrier_semaphore()
    peers = [jnp.where(j < me, j, j + 1) for j in range(n_seq - 1)]
    same = [low + pair * lax.rem(high + g, groups) for g in range(groups)]
    near = me < direct

    def greet(seq, hid):
        pl.semaphore_signal(barrier, inc=1, device_id=(seq, hid), device_id_type=MESH)

    for k in range(1, n_hid):
        greet(me, lax.rem(my_hid + k, n_hid))
    for p in peers:
        greet(p, my_hid)

    @pl.when(near)
    def _():
        for p in peers:
            for hid in same[1:]:
                greet(p, hid)

    if pair == 2:

        @pl.when((me == 0) & (my_hid == 1))
        def _():
            for p in range(n_seq):
                for g in range(groups):
                    greet(p, pair * g)

    smalls[0].wait()
    row = lax.broadcasted_iota(jnp.int32, (n_seq * block, 1), 0)
    inner = lax.rem(row, block)
    row_slot = (row // block) * per_owner + lax.rem(inner, per_owner)
    row_part = inner // per_owner
    doc = lax.broadcasted_iota(jnp.int32, (1, docs), 1)
    here = row_slot == slots[...]
    row_doc = jnp.sum(jnp.where(here, doc.astype(jnp.float32), 0.0), axis=1, keepdims=True).astype(jnp.int32)
    smalls[1].wait()
    pickers = [
        jnp.concatenate(
            [
                jnp.where(
                    jnp.where(row_part == f, row_doc, -1) == seg[k : k + 1, :], 1.0, 0.0
                ).astype(jnp.bfloat16)
                for k in range(tokens // LANES)
            ],
            axis=1,
        )
        for f in range(fold)
    ]
    smalls[2].wait()
    smalls[3].wait()
    length = lens[...].astype(jnp.float32)
    row_len = jnp.sum(jnp.where(here, length, 0.0), axis=1, keepdims=True)
    row_first = jnp.sum(jnp.where(doc < row_doc, length, 0.0), axis=1, keepdims=True)
    first = (me * tokens).astype(jnp.float32)
    starts = jnp.where((row_first >= first) & (row_first < first + tokens), 1.0, 0.0)
    inverse = 1.0 / row_len
    block_part = lax.broadcasted_iota(jnp.int32, (block, 1), 0) // per_owner
    offset = bias[:, :part]
    for f in range(1, fold):
        offset = jnp.where(block_part == f, bias[:, f * part : (f + 1) * part], offset)

    sums = None
    for t in range(chunks):
        loads[t].wait()
        for f in range(fold):
            term = jnp.dot(
                pickers[f][:, t * rows : (t + 1) * rows],
                hidden[t * rows : (t + 1) * rows, f * part : (f + 1) * part],
                preferred_element_type=jnp.float32,
            )
            sums = term if sums is None else sums + term

    for p in range(n_seq):
        at = slice(p * block, (p + 1) * block)
        share = sums[at] * inverse[at] + starts[at] * offset
        for j, tile in enumerate(narrowed(share)):
            code[p, :, j * LANES : (j + 1) * LANES] = tile

    pl.semaphore_wait(
        barrier,
        n_hid - 1 + n_seq - 1
        + (direct - jnp.where(near, 1, 0)) * (groups - 1)
        + jnp.where(low == 0, pair - 1, 0),
    )

    def send(p, hid, g):
        pltpu.make_async_remote_copy(
            src_ref=code.at[p],
            dst_ref=land.at[g, me],
            send_sem=send_sems.at[g],
            recv_sem=recv_sems.at[g],
            device_id=(p, hid),
            device_id_type=MESH,
        ).start()

    def send_extra():
        pltpu.make_async_remote_copy(
            src_ref=code.at[0],
            dst_ref=extra.at[high, me],
            send_sem=extra_send,
            recv_sem=extra_recv,
            device_id=(0, 1),
            device_id_type=MESH,
        ).start()

    for p in range(n_seq):

        @pl.when(p != me)
        def _():
            if p < direct:
                for i in range(groups):
                    send(p, low + pair * i, lax.rem(high - i + groups, groups))
            else:
                send(p, my_hid, 0)

        if p < direct:

            @pl.when(p == me)
            def _():
                for g in range(1, groups):
                    send(p, same[g], groups - g)

        if p == 0 and pair == 2:
            pl.when(low == 0)(send_extra)
    land[0, me] = code[me]

    most = land.at[0, pl.ds(0, n_seq - 1)]
    pltpu.make_async_copy(most, most, recv_sems.at[0]).wait()
    averages = summed(land, 0)
    lane_sq = squared(averages)
    ahead = (me == 0) & (my_hid == 0)
    alone = (me == 0) & (my_hid == 1)

    def pass_on(hid, k):
        return pltpu.make_async_remote_copy(
            src_ref=mine,
            dst_ref=theirs.at[k],
            send_sem=sq_send,
            recv_sem=sq_recv,
            device_id=(me, hid),
            device_id_type=MESH,
        )

    @pl.when(near)
    def _():
        both = lane_sq
        for g in range(1, groups):
            pltpu.make_async_copy(land.at[g], land.at[g], recv_sems.at[g]).wait()
            both = both + squared(summed(land, g))
        if pair == 2:
            mine[...] = both
            pl.when(jnp.logical_not(ahead))(pass_on(my_hid + 1 - 2 * low, 0).start)

            @pl.when(alone)
            def _():
                pltpu.make_async_copy(extra, extra, extra_recv).wait()
                rest = squared(summed(extra, 0))
                for g in range(1, groups):
                    rest = rest + squared(summed(extra, g))
                theirs[0] = rest

            @pl.when(jnp.logical_not(alone))
            def _():
                pltpu.make_async_copy(theirs.at[0], theirs.at[0], sq_recv).wait()

            both = both + theirs[0]
        whole[...] = both

    @pl.when(jnp.logical_not(near))
    def _():
        mine[...] = lane_sq
        for k in range(1, n_hid):
            pass_on(lax.rem(my_hid + k, n_hid), k - 1).start()
        pltpu.make_async_copy(theirs, theirs, sq_recv).wait()
        both = lane_sq
        for k in range(n_hid - 1):
            both = both + theirs[k]
        whole[...] = both

    lane_sq = whole[...]
    energy = jnp.sum(lane_sq, axis=1, keepdims=True)
    total = energy[:per_owner]
    for f in range(1, fold):
        total = total + energy[f * per_owner : (f + 1) * per_owner]
    scale = lax.rsqrt(total / features + 1e-06)
    for f in range(fold):
        for j, tile in enumerate(averages):
            at = f * part + j * LANES
            out_ref[:, at : at + LANES] = (tile[f * per_owner : (f + 1) * per_owner] * scale).astype(jnp.bfloat16)

    pltpu.make_async_copy(most, most, send_sems.at[0]).wait()
    for g in range(1, groups):
        sent = land.at[g, pl.ds(0, direct)]
        pltpu.make_async_copy(sent, sent, send_sems.at[g]).wait()
    if pair == 2:

        @pl.when(low == 0)
        def _():
            pltpu.make_async_copy(code.at[0], code.at[0], extra_send).wait()

        @pl.when(near & jnp.logical_not(ahead))
        def _():
            pltpu.make_async_copy(mine, mine, sq_send).wait()

    @pl.when(jnp.logical_not(near))
    def _():
        pltpu.make_async_copy(theirs, theirs, sq_send).wait()


def local(n_seq, n_hid, hidden, seg_ids, lengths, owner_slot, pool_bias):
    tokens, width = hidden.shape
    docs = lengths.shape[0]
    per_owner = docs // n_seq
    fold = max(1, 8 // per_owner)
    pair = 2 if n_hid % 2 == 0 else 1
    groups = n_hid // pair
    block, part = per_owner * fold, width // fold
    chunks = 4
    direct = max(1, n_seq // 2)
    f32, i32, i16 = jnp.float32, jnp.int32, jnp.int16
    dma = pltpu.SemaphoreType.DMA
    vmem = pltpu.VMEM
    return pl.pallas_call(
        functools.partial(kernel, n_seq, n_hid, pair, fold, chunks, direct),
        out_shape=vmem((per_owner, width), jnp.bfloat16),
        in_specs=[pl.BlockSpec(memory_space=pl.ANY)] * 5,
        out_specs=pl.BlockSpec(memory_space=vmem),
        scratch_shapes=[
            vmem((tokens, width), jnp.bfloat16),
            vmem((tokens // LANES, LANES), i32),
            vmem((1, docs), i32),
            vmem((1, docs), i32),
            vmem((1, width), f32),
            vmem((n_seq, block, part), i16),
            vmem((groups, n_seq, block, part), i16),
            vmem((groups, n_seq, block, part), i16),
            vmem((block, LANES), f32),
            vmem((n_hid - 1, block, LANES), f32),
            vmem((block, LANES), f32),
            dma((chunks,)),
            dma((4,)),
            dma((groups,)),
            dma((groups,)),
            dma(()),
            dma(()),
            dma(()),
            dma(()),
        ],
        compiler_params=pltpu.CompilerParams(collective_id=0, has_side_effects=True),
    )(
        hidden,
        seg_ids.reshape(tokens // LANES, LANES),
        lengths.reshape(1, docs),
        owner_slot.reshape(1, docs),
        pool_bias.reshape(1, width),
    )


def solution(mesh):
    placed = (P("seq", "hid"), P("seq"), P(), P(), P("hid"))
    return jax.shard_map(
        functools.partial(local, mesh.shape["seq"], mesh.shape["hid"]),
        mesh=mesh,
        in_specs=placed,
        out_specs=P("seq", "hid"),
        check_vma=False,
    )
```

```python
import functools

import jax
import jax.numpy as jnp
from jax import lax
from jax.experimental import pallas as pl
from jax.experimental.pallas import tpu as pltpu
from jax.sharding import PartitionSpec as P

MESH = pl.DeviceIdType.MESH
LANES = 128
STEPS = 8.0
LEAST = 20.0
STEP_BITS = 8


def widened(code):
    tiles = code.shape[1] // LANES
    low = -(-STEP_BITS // tiles)
    top = float((1 << (15 - low)) - 24)
    words = [code[:, j * LANES : (j + 1) * LANES].astype(jnp.int32) for j in range(tiles)]
    step = words[0] & ((1 << low) - 1)
    for j in range(1, tiles):
        step = step | ((words[j] & ((1 << low) - 1)) << (low * j))
    unit = jnp.exp2(step.astype(jnp.float32) * (1.0 / STEPS) - LEAST) * (1.0 / top)
    return [(w >> low).astype(jnp.float32) * unit for w in words]


def narrowed(share):
    tiles = share.shape[1] // LANES
    low = -(-STEP_BITS // tiles)
    top = float((1 << (15 - low)) - 24)
    parts = [share[:, j * LANES : (j + 1) * LANES] for j in range(tiles)]
    largest = jnp.abs(parts[0])
    for x in parts[1:]:
        largest = jnp.maximum(largest, jnp.abs(x))
    step = jnp.ceil((jnp.log2(jnp.maximum(largest, 2.0**-LEAST)) + LEAST) * STEPS)
    gain = jnp.exp2(LEAST - step * (1.0 / STEPS)) * top
    bits = step.astype(jnp.int32)
    return [
        (
            (jnp.round(x * gain).astype(jnp.int32) << low) | ((bits >> (low * j)) & ((1 << low) - 1))
        ).astype(jnp.int16)
        for j, x in enumerate(parts)
    ]


def summed(land, group):
    total = widened(land[group, 0])
    for k in range(1, land.shape[1]):
        total = [a + b for a, b in zip(total, widened(land[group, k]))]
    return total


def squared(tiles):
    out = tiles[0] * tiles[0]
    for t in tiles[1:]:
        out = out + t * t
    return out


def kernel(
    n_seq, n_hid, pair, fold, chunks, direct,
    hidden_hbm, seg_hbm, len_hbm, slot_hbm, bias_hbm,
    out_ref,
    hidden, seg, lens, slots, bias, code, land, extra, mine, theirs, whole,
    load_sems, small_sems, send_sems, recv_sems, extra_send, extra_recv, sq_send, sq_recv,
):
    me = lax.axis_index("seq")
    my_hid = lax.axis_index("hid")
    tokens, width = hidden.shape
    docs = lens.shape[1]
    per_owner = docs // n_seq
    block = per_owner * fold
    part = width // fold
    groups = n_hid // pair
    low = lax.rem(my_hid, pair)
    high = my_hid // pair
    features = width * n_hid

    rows = tokens // chunks
    smalls = [
        pltpu.make_async_copy(src, dst, small_sems.at[i])
        for i, (src, dst) in enumerate(
            ((slot_hbm, slots), (seg_hbm, seg), (len_hbm, lens), (bias_hbm, bias))
        )
    ]
    loads = [
        pltpu.make_async_copy(
            hidden_hbm.at[pl.ds(t * rows, rows), :], hidden.at[pl.ds(t * rows, rows), :], load_sems.at[t]
        )
        for t in range(chunks)
    ]
    for c in smalls:
        c.start()
    for c in loads:
        c.start()

    barrier = pltpu.get_barrier_semaphore()
    peers = [jnp.where(j < me, j, j + 1) for j in range(n_seq - 1)]
    same = [low + pair * lax.rem(high + g, groups) for g in range(groups)]
    near = me < direct

    def greet(seq, hid):
        pl.semaphore_signal(barrier, inc=1, device_id=(seq, hid), device_id_type=MESH)

    for k in range(1, n_hid):
        greet(me, lax.rem(my_hid + k, n_hid))
    for p in peers:
        greet(p, my_hid)

    @pl.when(near)
    def _():
        for p in peers:
            for hid in same[1:]:
                greet(p, hid)

    if pair == 2:

        @pl.when((me == 0) & (my_hid == 1))
        def _():
            for p in range(n_seq):
                for g in range(groups):
                    greet(p, pair * g)

    smalls[0].wait()
    row = lax.broadcasted_iota(jnp.int32, (n_seq * block, 1), 0)
    inner = lax.rem(row, block)
    row_slot = (row // block) * per_owner + lax.rem(inner, per_owner)
    row_part = inner // per_owner
    doc = lax.broadcasted_iota(jnp.int32, (1, docs), 1)
    here = row_slot == slots[...]
    row_doc = jnp.sum(jnp.where(here, doc.astype(jnp.float32), 0.0), axis=1, keepdims=True).astype(jnp.int32)
    smalls[1].wait()
    pickers = [
        jnp.concatenate(
            [
                jnp.where(
                    jnp.where(row_part == f, row_doc, -1) == seg[k : k + 1, :], 1.0, 0.0
                ).astype(jnp.bfloat16)
                for k in range(tokens // LANES)
            ],
            axis=1,
        )
        for f in range(fold)
    ]
    sums = None
    for t in range(2):
        loads[t].wait()
        for f in range(fold):
            term = jnp.dot(
                pickers[f][:, t * rows : (t + 1) * rows],
                hidden[t * rows : (t + 1) * rows, f * part : (f + 1) * part],
                preferred_element_type=jnp.float32,
            )
            sums = term if sums is None else sums + term
    smalls[2].wait()
    smalls[3].wait()
    length = lens[...].astype(jnp.float32)
    row_len = jnp.sum(jnp.where(here, length, 0.0), axis=1, keepdims=True)
    row_first = jnp.sum(jnp.where(doc < row_doc, length, 0.0), axis=1, keepdims=True)
    first = (me * tokens).astype(jnp.float32)
    starts = jnp.where((row_first >= first) & (row_first < first + tokens), 1.0, 0.0)
    inverse = 1.0 / row_len
    block_part = lax.broadcasted_iota(jnp.int32, (block, 1), 0) // per_owner
    offset = bias[:, :part]
    for f in range(1, fold):
        offset = jnp.where(block_part == f, bias[:, f * part : (f + 1) * part], offset)

    for t in range(2, chunks):
        loads[t].wait()
        for f in range(fold):
            term = jnp.dot(
                pickers[f][:, t * rows : (t + 1) * rows],
                hidden[t * rows : (t + 1) * rows, f * part : (f + 1) * part],
                preferred_element_type=jnp.float32,
            )
            sums = term if sums is None else sums + term

    for p in range(n_seq):
        at = slice(p * block, (p + 1) * block)
        share = sums[at] * inverse[at] + starts[at] * offset
        for j, tile in enumerate(narrowed(share)):
            code[p, :, j * LANES : (j + 1) * LANES] = tile

    pl.semaphore_wait(
        barrier,
        n_hid - 1 + n_seq - 1
        + (direct - jnp.where(near, 1, 0)) * (groups - 1)
        + jnp.where(low == 0, pair - 1, 0),
    )

    def send(p, hid, g):
        pltpu.make_async_remote_copy(
            src_ref=code.at[p],
            dst_ref=land.at[g, me],
            send_sem=send_sems.at[g],
            recv_sem=recv_sems.at[g],
            device_id=(p, hid),
            device_id_type=MESH,
        ).start()

    def send_extra():
        pltpu.make_async_remote_copy(
            src_ref=code.at[0],
            dst_ref=extra.at[high, me],
            send_sem=extra_send,
            recv_sem=extra_recv,
            device_id=(0, 1),
            device_id_type=MESH,
        ).start()

    def send_near(p):
        @pl.when(p != me)
        def _():
            for i in range(groups):
                send(p, low + pair * i, lax.rem(high - i + groups, groups))

        @pl.when(p == me)
        def _():
            for g in range(1, groups):
                send(p, same[g], groups - g)

    urgent = (direct + 1) // 2
    send_near(0)
    if pair == 2:
        pl.when(low == 0)(send_extra)
    for p in range(1, urgent):
        send_near(p)
    for p in range(direct, n_seq):
        pl.when(p != me)(functools.partial(send, p, my_hid, 0))
    for p in range(urgent, direct):
        send_near(p)

    land[0, me] = code[me]

    most = land.at[0, pl.ds(0, n_seq - 1)]
    pltpu.make_async_copy(most, most, recv_sems.at[0]).wait()
    averages = summed(land, 0)
    lane_sq = squared(averages)
    ahead = (me == 0) & (my_hid == 0)
    alone = (me == 0) & (my_hid == 1)

    def pass_on(hid, k):
        return pltpu.make_async_remote_copy(
            src_ref=mine,
            dst_ref=theirs.at[k],
            send_sem=sq_send,
            recv_sem=sq_recv,
            device_id=(me, hid),
            device_id_type=MESH,
        )

    @pl.when(near)
    def _():
        both = lane_sq
        for g in range(1, groups):
            pltpu.make_async_copy(land.at[g], land.at[g], recv_sems.at[g]).wait()
            both = both + squared(summed(land, g))
        if pair == 2:
            mine[...] = both
            pl.when(jnp.logical_not(ahead))(pass_on(my_hid + 1 - 2 * low, 0).start)

            @pl.when(alone)
            def _():
                pltpu.make_async_copy(extra, extra, extra_recv).wait()
                rest = squared(summed(extra, 0))
                for g in range(1, groups):
                    rest = rest + squared(summed(extra, g))
                theirs[0] = rest

            @pl.when(jnp.logical_not(alone))
            def _():
                pltpu.make_async_copy(theirs.at[0], theirs.at[0], sq_recv).wait()

            both = both + theirs[0]
        whole[...] = both

    @pl.when(jnp.logical_not(near))
    def _():
        mine[...] = lane_sq
        for k in range(1, n_hid):
            pass_on(lax.rem(my_hid + k, n_hid), k - 1).start()
        pltpu.make_async_copy(theirs, theirs, sq_recv).wait()
        both = lane_sq
        for k in range(n_hid - 1):
            both = both + theirs[k]
        whole[...] = both

    lane_sq = whole[...]
    energy = jnp.sum(lane_sq, axis=1, keepdims=True)
    total = energy[:per_owner]
    for f in range(1, fold):
        total = total + energy[f * per_owner : (f + 1) * per_owner]
    scale = lax.rsqrt(total / features + 1e-06)
    for f in range(fold):
        for j, tile in enumerate(averages):
            at = f * part + j * LANES
            out_ref[:, at : at + LANES] = (tile[f * per_owner : (f + 1) * per_owner] * scale).astype(jnp.bfloat16)

    pltpu.make_async_copy(most, most, send_sems.at[0]).wait()
    for g in range(1, groups):
        sent = land.at[g, pl.ds(0, direct)]
        pltpu.make_async_copy(sent, sent, send_sems.at[g]).wait()
    if pair == 2:

        @pl.when(low == 0)
        def _():
            pltpu.make_async_copy(code.at[0], code.at[0], extra_send).wait()

        @pl.when(near & jnp.logical_not(ahead))
        def _():
            pltpu.make_async_copy(mine, mine, sq_send).wait()

    @pl.when(jnp.logical_not(near))
    def _():
        pltpu.make_async_copy(theirs, theirs, sq_send).wait()


def local(n_seq, n_hid, hidden, seg_ids, lengths, owner_slot, pool_bias):
    tokens, width = hidden.shape
    docs = lengths.shape[0]
    per_owner = docs // n_seq
    fold = max(1, 8 // per_owner)
    pair = 2 if n_hid % 2 == 0 else 1
    groups = n_hid // pair
    block, part = per_owner * fold, width // fold
    chunks = 4
    direct = max(1, n_seq // 2)
    f32, i32, i16 = jnp.float32, jnp.int32, jnp.int16
    dma = pltpu.SemaphoreType.DMA
    vmem = pltpu.VMEM
    return pl.pallas_call(
        functools.partial(kernel, n_seq, n_hid, pair, fold, chunks, direct),
        out_shape=vmem((per_owner, width), jnp.bfloat16),
        in_specs=[pl.BlockSpec(memory_space=pl.ANY)] * 5,
        out_specs=pl.BlockSpec(memory_space=vmem),
        scratch_shapes=[
            vmem((tokens, width), jnp.bfloat16),
            vmem((tokens // LANES, LANES), i32),
            vmem((1, docs), i32),
            vmem((1, docs), i32),
            vmem((1, width), f32),
            vmem((n_seq, block, part), i16),
            vmem((groups, n_seq, block, part), i16),
            vmem((groups, n_seq, block, part), i16),
            vmem((block, LANES), f32),
            vmem((n_hid - 1, block, LANES), f32),
            vmem((block, LANES), f32),
            dma((chunks,)),
            dma((4,)),
            dma((groups,)),
            dma((groups,)),
            dma(()),
            dma(()),
            dma(()),
            dma(()),
        ],
        compiler_params=pltpu.CompilerParams(collective_id=0, has_side_effects=True),
    )(
        hidden,
        seg_ids.reshape(tokens // LANES, LANES),
        lengths.reshape(1, docs),
        owner_slot.reshape(1, docs),
        pool_bias.reshape(1, width),
    )


def solution(mesh):
    placed = (P("seq", "hid"), P("seq"), P(), P(), P("hid"))
    return jax.shard_map(
        functools.partial(local, mesh.shape["seq"], mesh.shape["hid"]),
        mesh=mesh,
        in_specs=placed,
        out_specs=P("seq", "hid"),
        check_vma=False,
    )
```

```python
import functools

import jax
import jax.numpy as jnp
from jax import lax
from jax.experimental import pallas as pl
from jax.experimental.pallas import tpu as pltpu
from jax.sharding import PartitionSpec as P

MESH = pl.DeviceIdType.MESH
LANES = 128
STEPS = 8.0
LEAST = 20.0
STEP_BITS = 8


def widened(code):
    tiles = code.shape[1] // LANES
    low = -(-STEP_BITS // tiles)
    top = float((1 << (15 - low)) - 24)
    words = [code[:, j * LANES : (j + 1) * LANES].astype(jnp.int32) for j in range(tiles)]
    step = words[0] & ((1 << low) - 1)
    for j in range(1, tiles):
        step = step | ((words[j] & ((1 << low) - 1)) << (low * j))
    unit = jnp.exp2(step.astype(jnp.float32) * (1.0 / STEPS) - LEAST) * (1.0 / top)
    return [(w >> low).astype(jnp.float32) * unit for w in words]


def narrowed(share):
    tiles = share.shape[1] // LANES
    low = -(-STEP_BITS // tiles)
    top = float((1 << (15 - low)) - 24)
    parts = [share[:, j * LANES : (j + 1) * LANES] for j in range(tiles)]
    largest = jnp.abs(parts[0])
    for x in parts[1:]:
        largest = jnp.maximum(largest, jnp.abs(x))
    step = jnp.ceil((jnp.log2(jnp.maximum(largest, 2.0**-LEAST)) + LEAST) * STEPS)
    gain = jnp.exp2(LEAST - step * (1.0 / STEPS)) * top
    bits = step.astype(jnp.int32)
    return [
        (
            (jnp.round(x * gain).astype(jnp.int32) << low) | ((bits >> (low * j)) & ((1 << low) - 1))
        ).astype(jnp.int16)
        for j, x in enumerate(parts)
    ]


def summed(land, group):
    total = widened(land[group, 0])
    for k in range(1, land.shape[1]):
        total = [a + b for a, b in zip(total, widened(land[group, k]))]
    return total


def squared(tiles):
    out = tiles[0] * tiles[0]
    for t in tiles[1:]:
        out = out + t * t
    return out


def kernel(
    n_seq, n_hid, pair, fold, chunks, direct,
    hidden_hbm, seg_hbm, len_hbm, slot_hbm, bias_hbm,
    out_ref,
    hidden, seg, lens, slots, bias, code, land, extra, mine, theirs, whole,
    load_sems, small_sems, send_sems, recv_sems, extra_send, extra_recv, sq_send, sq_recv,
):
    me = lax.axis_index("seq")
    my_hid = lax.axis_index("hid")
    tokens, width = hidden.shape
    docs = lens.shape[1]
    per_owner = docs // n_seq
    block = per_owner * fold
    part = width // fold
    groups = n_hid // pair
    low = lax.rem(my_hid, pair)
    high = my_hid // pair
    features = width * n_hid

    rows = tokens // chunks
    smalls = [
        pltpu.make_async_copy(src, dst, small_sems.at[i])
        for i, (src, dst) in enumerate(
            ((slot_hbm, slots), (seg_hbm, seg), (len_hbm, lens), (bias_hbm, bias))
        )
    ]
    loads = [
        pltpu.make_async_copy(
            hidden_hbm.at[pl.ds(t * rows, rows), :], hidden.at[pl.ds(t * rows, rows), :], load_sems.at[t]
        )
        for t in range(chunks)
    ]
    for c in smalls:
        c.start()
    for c in loads:
        c.start()

    barrier = pltpu.get_barrier_semaphore()
    peers = [jnp.where(j < me, j, j + 1) for j in range(n_seq - 1)]
    same = [low + pair * lax.rem(high + g, groups) for g in range(groups)]
    near = me < direct

    def greet(seq, hid):
        pl.semaphore_signal(barrier, inc=1, device_id=(seq, hid), device_id_type=MESH)

    for k in range(1, n_hid):
        greet(me, lax.rem(my_hid + k, n_hid))
    for p in peers:
        greet(p, my_hid)

    @pl.when(near)
    def _():
        for p in peers:
            for hid in same[1:]:
                greet(p, hid)

    if pair == 2:

        @pl.when((me == 0) & (my_hid == 1))
        def _():
            for p in range(n_seq):
                for g in range(groups):
                    greet(p, pair * g)

    smalls[0].wait()
    row = lax.broadcasted_iota(jnp.int32, (n_seq * block, 1), 0)
    inner = lax.rem(row, block)
    row_slot = (row // block) * per_owner + lax.rem(inner, per_owner)
    row_part = inner // per_owner
    doc = lax.broadcasted_iota(jnp.int32, (1, docs), 1)
    here = row_slot == slots[...]
    row_doc = jnp.sum(jnp.where(here, doc.astype(jnp.float32), 0.0), axis=1, keepdims=True).astype(jnp.int32)
    smalls[1].wait()
    pickers = [
        jnp.concatenate(
            [
                jnp.where(
                    jnp.where(row_part == f, row_doc, -1) == seg[k : k + 1, :], 1.0, 0.0
                ).astype(jnp.bfloat16)
                for k in range(tokens // LANES)
            ],
            axis=1,
        )
        for f in range(fold)
    ]
    sums = None
    for t in range(2):
        loads[t].wait()
        for f in range(fold):
            term = jnp.dot(
                pickers[f][:, t * rows : (t + 1) * rows],
                hidden[t * rows : (t + 1) * rows, f * part : (f + 1) * part],
                preferred_element_type=jnp.float32,
            )
            sums = term if sums is None else sums + term
    smalls[2].wait()
    smalls[3].wait()
    length = lens[...].astype(jnp.float32)
    row_len = jnp.sum(jnp.where(here, length, 0.0), axis=1, keepdims=True)
    row_first = jnp.sum(jnp.where(doc < row_doc, length, 0.0), axis=1, keepdims=True)
    first = (me * tokens).astype(jnp.float32)
    starts = jnp.where((row_first >= first) & (row_first < first + tokens), 1.0, 0.0)
    inverse = 1.0 / row_len
    block_part = lax.broadcasted_iota(jnp.int32, (block, 1), 0) // per_owner
    offset = bias[:, :part]
    for f in range(1, fold):
        offset = jnp.where(block_part == f, bias[:, f * part : (f + 1) * part], offset)

    for t in range(2, chunks):
        loads[t].wait()
        for f in range(fold):
            term = jnp.dot(
                pickers[f][:, t * rows : (t + 1) * rows],
                hidden[t * rows : (t + 1) * rows, f * part : (f + 1) * part],
                preferred_element_type=jnp.float32,
            )
            sums = term if sums is None else sums + term

    def send(p, hid, g):
        pltpu.make_async_remote_copy(
            src_ref=code.at[p],
            dst_ref=land.at[g, me],
            send_sem=send_sems.at[g],
            recv_sem=recv_sems.at[g],
            device_id=(p, hid),
            device_id_type=MESH,
        ).start()

    def send_extra():
        pltpu.make_async_remote_copy(
            src_ref=code.at[0],
            dst_ref=extra.at[high, me],
            send_sem=extra_send,
            recv_sem=extra_recv,
            device_id=(0, 1),
            device_id_type=MESH,
        ).start()

    def send_near(p):
        @pl.when(p != me)
        def _():
            for i in range(groups):
                send(p, low + pair * i, lax.rem(high - i + groups, groups))

        @pl.when(p == me)
        def _():
            for g in range(1, groups):
                send(p, same[g], groups - g)

    for p in range(2):
        at = slice(p * block, (p + 1) * block)
        share = sums[at] * inverse[at] + starts[at] * offset
        for j, tile in enumerate(narrowed(share)):
            code[p, :, j * LANES : (j + 1) * LANES] = tile

    pl.semaphore_wait(
        barrier,
        n_hid - 1 + n_seq - 1
        + (direct - jnp.where(near, 1, 0)) * (groups - 1)
        + jnp.where(low == 0, pair - 1, 0),
    )

    urgent = (direct + 1) // 2
    send_near(0)
    if pair == 2:
        pl.when(low == 0)(send_extra)
    for p in range(2, n_seq):
        at = slice(p * block, (p + 1) * block)
        share = sums[at] * inverse[at] + starts[at] * offset
        for j, tile in enumerate(narrowed(share)):
            code[p, :, j * LANES : (j + 1) * LANES] = tile

    for p in range(1, urgent):
        send_near(p)
    for p in range(direct, n_seq):
        pl.when(p != me)(functools.partial(send, p, my_hid, 0))
    for p in range(urgent, direct):
        send_near(p)

    land[0, me] = code[me]

    most = land.at[0, pl.ds(0, n_seq - 1)]
    pltpu.make_async_copy(most, most, recv_sems.at[0]).wait()
    averages = summed(land, 0)
    lane_sq = squared(averages)
    ahead = (me == 0) & (my_hid == 0)
    alone = (me == 0) & (my_hid == 1)

    def pass_on(hid, k):
        return pltpu.make_async_remote_copy(
            src_ref=mine,
            dst_ref=theirs.at[k],
            send_sem=sq_send,
            recv_sem=sq_recv,
            device_id=(me, hid),
            device_id_type=MESH,
        )

    @pl.when(near)
    def _():
        both = lane_sq
        for g in range(1, groups):
            pltpu.make_async_copy(land.at[g], land.at[g], recv_sems.at[g]).wait()
            both = both + squared(summed(land, g))
        if pair == 2:
            mine[...] = both
            pl.when(jnp.logical_not(ahead))(pass_on(my_hid + 1 - 2 * low, 0).start)

            @pl.when(alone)
            def _():
                pltpu.make_async_copy(extra, extra, extra_recv).wait()
                rest = squared(summed(extra, 0))
                for g in range(1, groups):
                    rest = rest + squared(summed(extra, g))
                theirs[0] = rest

            @pl.when(jnp.logical_not(alone))
            def _():
                pltpu.make_async_copy(theirs.at[0], theirs.at[0], sq_recv).wait()

            both = both + theirs[0]
        whole[...] = both

    @pl.when(jnp.logical_not(near))
    def _():
        mine[...] = lane_sq
        for k in range(1, n_hid):
            pass_on(lax.rem(my_hid + k, n_hid), k - 1).start()
        pltpu.make_async_copy(theirs, theirs, sq_recv).wait()
        both = lane_sq
        for k in range(n_hid - 1):
            both = both + theirs[k]
        whole[...] = both

    lane_sq = whole[...]
    energy = jnp.sum(lane_sq, axis=1, keepdims=True)
    total = energy[:per_owner]
    for f in range(1, fold):
        total = total + energy[f * per_owner : (f + 1) * per_owner]
    scale = lax.rsqrt(total / features + 1e-06)
    for f in range(fold):
        for j, tile in enumerate(averages):
            at = f * part + j * LANES
            out_ref[:, at : at + LANES] = (tile[f * per_owner : (f + 1) * per_owner] * scale).astype(jnp.bfloat16)

    pltpu.make_async_copy(most, most, send_sems.at[0]).wait()
    for g in range(1, groups):
        sent = land.at[g, pl.ds(0, direct)]
        pltpu.make_async_copy(sent, sent, send_sems.at[g]).wait()
    if pair == 2:

        @pl.when(low == 0)
        def _():
            pltpu.make_async_copy(code.at[0], code.at[0], extra_send).wait()

        @pl.when(near & jnp.logical_not(ahead))
        def _():
            pltpu.make_async_copy(mine, mine, sq_send).wait()

    @pl.when(jnp.logical_not(near))
    def _():
        pltpu.make_async_copy(theirs, theirs, sq_send).wait()


def local(n_seq, n_hid, hidden, seg_ids, lengths, owner_slot, pool_bias):
    tokens, width = hidden.shape
    docs = lengths.shape[0]
    per_owner = docs // n_seq
    fold = max(1, 8 // per_owner)
    pair = 2 if n_hid % 2 == 0 else 1
    groups = n_hid // pair
    block, part = per_owner * fold, width // fold
    chunks = 4
    direct = max(1, n_seq // 2)
    f32, i32, i16 = jnp.float32, jnp.int32, jnp.int16
    dma = pltpu.SemaphoreType.DMA
    vmem = pltpu.VMEM
    return pl.pallas_call(
        functools.partial(kernel, n_seq, n_hid, pair, fold, chunks, direct),
        out_shape=vmem((per_owner, width), jnp.bfloat16),
        in_specs=[pl.BlockSpec(memory_space=pl.ANY)] * 5,
        out_specs=pl.BlockSpec(memory_space=vmem),
        scratch_shapes=[
            vmem((tokens, width), jnp.bfloat16),
            vmem((tokens // LANES, LANES), i32),
            vmem((1, docs), i32),
            vmem((1, docs), i32),
            vmem((1, width), f32),
            vmem((n_seq, block, part), i16),
            vmem((groups, n_seq, block, part), i16),
            vmem((groups, n_seq, block, part), i16),
            vmem((block, LANES), f32),
            vmem((n_hid - 1, block, LANES), f32),
            vmem((block, LANES), f32),
            dma((chunks,)),
            dma((4,)),
            dma((groups,)),
            dma((groups,)),
            dma(()),
            dma(()),
            dma(()),
            dma(()),
        ],
        compiler_params=pltpu.CompilerParams(collective_id=0, has_side_effects=True),
    )(
        hidden,
        seg_ids.reshape(tokens // LANES, LANES),
        lengths.reshape(1, docs),
        owner_slot.reshape(1, docs),
        pool_bias.reshape(1, width),
    )


def solution(mesh):
    placed = (P("seq", "hid"), P("seq"), P(), P(), P("hid"))
    return jax.shard_map(
        functools.partial(local, mesh.shape["seq"], mesh.shape["hid"]),
        mesh=mesh,
        in_specs=placed,
        out_specs=P("seq", "hid"),
        check_vma=False,
    )
```
